8 devices in a mesh: dp: 1 (over z), ep: 8 (over y, x, core).
Axes of the slice: x: 2, y: 2, z: 1, core: 2. Of those that a mesh axis runs over, the one named last changes fastest.
Arguments:
- tokens: bfloat16 [32768, 2048], P(('dp', 'ep'))
- topk_idx: int32 [32768, 2], P(('dp', 'ep'))
- topk_w: float32 [32768, 2], P(('dp', 'ep'))
- w_up: bfloat16 [8, 2, 2048, 5632], P('ep')
- w_down: bfloat16 [8, 2, 5632, 2048], P('ep')
- slot_expert: int32 [8, 2], replicated
Outputs:
- output: bfloat16 [32768, 2048], P(('dp', 'ep'))
All inputs are finite; a program needn't handle non-finite values.
Results may differ from the reference program's by a relative error of at most 0.00133.
Values are sent between devices in bfloat16 or wider.
A program may use at most 1 GiB of HBM per device.

```python
import jax
import jax.numpy as jnp
from jax import lax
import numpy as np

GROUP = 8
TOK_DEV = 4096
D_MODEL = 2048
D_FF = 5632
EXPERTS = 8
TOP = 2

PER_DEV = EXPERTS // GROUP
SLOTS = PER_DEV + 1
N_UNITS = GROUP * SLOTS
PAIRS_DEV = TOK_DEV * TOP
BASE_LOAD = PAIRS_DEV // N_UNITS
BLOCK = max(8, (GROUP * PAIRS_DEV) // N_UNITS)
N_BLOCKS = (GROUP * PAIRS_DEV) // BLOCK + EXPERTS


def base_table():
    dev_ids = np.arange(GROUP)
    hot_dev = (3 * (dev_ids // 3) + 3) % GROUP
    spare_exp = hot_dev * PER_DEV + PER_DEV - 1
    primary = np.arange(EXPERTS).reshape(GROUP, PER_DEV)
    return np.concatenate([primary, spare_exp[:, None]], axis=1).astype(np.int32)


def draw_table(key_tab):
    key_dev, key_col, key_lab = jax.random.split(key_tab, 3)
    relabel = jax.random.permutation(key_lab, EXPERTS).astype(jnp.int32)
    dev_perm = jax.random.permutation(key_dev, GROUP)
    col_perm = jax.random.permutation(key_col, SLOTS)
    slot_table = jnp.asarray(base_table())[dev_perm][:, col_perm]
    return relabel[slot_table], relabel


def draw_loads(key_load):
    key_perm, key_shift = jax.random.split(key_load)
    unit_order = 1 + jax.random.permutation(key_perm, N_UNITS - 1)
    shift_amt = jax.random.randint(key_shift, ((N_UNITS - 2) // 2,), 0, BASE_LOAD // 2 + 1, dtype=jnp.int32)
    spread = BASE_LOAD // 2 + 1
    unit_loads = jnp.full((N_UNITS,), BASE_LOAD, jnp.int32)
    unit_loads = unit_loads.at[0].add(spread).at[unit_order[0]].add(-spread)
    unit_loads = unit_loads.at[unit_order[1::2]].add(shift_amt).at[unit_order[2::2]].add(-shift_amt)
    return unit_loads.at[unit_order[:PAIRS_DEV - N_UNITS * BASE_LOAD]].add(1)


def draw_routing(key_src, unit_expert):
    key_load, key_tok = jax.random.split(key_src)
    counts = jax.ops.segment_sum(draw_loads(key_load), unit_expert, num_segments=EXPERTS)
    bounds = jnp.cumsum(counts)
    sorted_exp = jnp.searchsorted(bounds, jnp.arange(PAIRS_DEV, dtype=jnp.int32), side='right').astype(jnp.int32)
    routes = sorted_exp.reshape(TOP, TOK_DEV).T
    return routes[jax.random.permutation(key_tok, TOK_DEV)]


def setup_inputs(seed: int = 0, part: int = 0) -> dict:
    root_key = jax.random.key(seed)
    key_tab, key_up, key_down, key_part = jax.random.split(root_key, 4)
    slot_expert, relabel = draw_table(key_tab)
    unit_expert = relabel[jnp.asarray(base_table()).reshape(-1)]
    up_base = jax.random.normal(key_up, (EXPERTS, D_MODEL, D_FF), jnp.float32) * D_MODEL ** -0.5
    down_base = jax.random.normal(key_down, (EXPERTS, D_FF, D_MODEL), jnp.float32) * D_FF ** -0.5
    key_grp = jax.random.fold_in(key_part, part)
    key_tokens, key_gate, key_route = jax.random.split(key_grp, 3)
    tokens = jax.random.normal(key_tokens, (GROUP * TOK_DEV, D_MODEL), jnp.float32)
    topk_w = jax.random.uniform(key_gate, (GROUP * TOK_DEV, TOP), jnp.float32, 0.3, 1.0)
    src_keys = jax.random.split(key_route, GROUP)
    topk_idx = jax.vmap(draw_routing, in_axes=(0, None))(src_keys, unit_expert)
    return {'tokens': tokens.astype(jnp.bfloat16), 'topk_idx': topk_idx.reshape(GROUP * TOK_DEV, TOP), 'topk_w': topk_w, 'w_up': up_base.astype(jnp.bfloat16)[slot_expert], 'w_down': down_base.astype(jnp.bfloat16)[slot_expert], 'slot_expert': slot_expert}


def reference(tokens, topk_idx, topk_w, w_up, w_down, slot_expert):
    n_tok = tokens.shape[0]
    n_pairs = n_tok * TOP
    table_flat = slot_expert.reshape(-1)
    first_slot = jax.ops.segment_min(jnp.arange(N_UNITS, dtype=jnp.int32), table_flat, num_segments=EXPERTS)
    up_flat = w_up.reshape(N_UNITS, D_MODEL, D_FF)
    down_flat = w_down.reshape(N_UNITS, D_FF, D_MODEL)
    flat_exp = topk_idx.reshape(-1)
    flat_gate = topk_w.reshape(-1)
    pair_order = jnp.argsort(flat_exp, stable=True)
    counts = jnp.bincount(flat_exp, length=EXPERTS)
    starts = jnp.cumsum(counts) - counts
    exp_blocks = (counts + BLOCK - 1) // BLOCK
    block_end = jnp.cumsum(exp_blocks)
    block_start = block_end - exp_blocks
    lane_ids = jnp.arange(BLOCK)

    def block_step(acc_sum, block_id):
        exp_id = jnp.minimum(jnp.searchsorted(block_end, block_id, side='right'), EXPERTS - 1)
        offsets = (block_id - block_start[exp_id]) * BLOCK + lane_ids
        is_valid = (offsets < counts[exp_id]) & (block_id < block_end[EXPERTS - 1])
        pair_ids = pair_order[jnp.clip(starts[exp_id] + offsets, 0, n_pairs - 1)]
        tok_ids = pair_ids // TOP
        slot_id = first_slot[exp_id]
        pre_act = jnp.dot(tokens[tok_ids], up_flat[slot_id], preferred_element_type=jnp.float32)
        hidden = jax.nn.gelu(pre_act, approximate=True).astype(jnp.bfloat16)
        expert_out = jnp.dot(hidden, down_flat[slot_id], preferred_element_type=jnp.float32).astype(jnp.bfloat16)
        gate_vals = jnp.where(is_valid, flat_gate[pair_ids], 0.0)
        return acc_sum.at[tok_ids].add(gate_vals[:, None] * expert_out.astype(jnp.float32)), None

    acc_out, _ = lax.scan(block_step, jnp.zeros((n_tok, D_MODEL), jnp.float32), jnp.arange(N_BLOCKS))
    return acc_out.astype(jnp.bfloat16)
```

```python
import functools

import jax
import jax.numpy as jnp
from jax import lax
from jax.experimental import pallas as pl
from jax.experimental.pallas import tpu as pltpu
from jax.sharding import PartitionSpec as P


GROUP = 16
N_DEV = 8
N_CHIP = 4
N_SLOT = 2
N_EXP = 8
N_UNIT = N_DEV * N_SLOT
N_PIECE = 7
TILE_G = 32
TILE_M = TILE_G * GROUP
TILE_F = 512
SWEEPS = 3
LANE = 128
CLASSES = (2, 4, 6, 7, 3, 5)
BATCHES = ((0, 1), (2, 3), (4, 5))
CAP_GRPS = (49, 56, 98)
LOCAL_GRPS = 520
MAX_T = 20
MAX_E = MAX_T * TILE_G
N_CALL = 2 + len(BATCHES)
AID = 4096
VMEM_BYTES = 60 * 1024 * 1024


def plan_kernel(me_ref, cnt_ref, slot_ref, cls_ref, piece_at, piece_add, pick_ref, *refs):
    ents, units, cnts, nts = (refs[i * N_CALL:(i + 1) * N_CALL] for i in range(4))
    grp, has, opts, chip_k, x = refs[4 * N_CALL:]
    i32 = jnp.int32
    me = me_ref[0]
    chip = me // 2
    core = me % 2

    def X(p, c, e):
        return (p * N_CHIP + c) * N_EXP + e

    @pl.loop(0, N_CHIP * N_EXP)
    def _(i):
        has[i] = i32(0)

    @pl.loop(0, N_EXP)
    def _(i):
        opts[i] = i32(0)

    @pl.loop(0, N_UNIT)
    def _(k):
        e = slot_ref[k]
        i = (k // 4) * N_EXP + e
        has[i] = has[i] + 1
        opts[e] = opts[e] + 1

    @pl.loop(0, N_DEV * N_EXP)
    def _(i):
        g = (cnt_ref[i] + (GROUP - 1)) // GROUP
        grp[i] = g
        p = i // N_EXP
        e = i % N_EXP
        own = p // 2
        at_home = has[own * N_EXP + e] > 0
        left = g
        for c in range(N_CHIP):
            here = jnp.where(at_home, own == c, has[c * N_EXP + e] > 0)
            amt = jnp.where(here, left, 0)
            x[X(p, c, e)] = amt
            left = left - amt

    def chip_sums():
        @pl.loop(0, N_DEV * N_CHIP)
        def _(i):
            def add(e, acc):
                return acc + x[i * N_EXP + e]
            chip_k[i] = lax.fori_loop(0, N_EXP, add, i32(0))

    chip_sums()

    @pl.loop(0, N_DEV * SWEEPS)
    def _(i):
        p = i // SWEEPS
        own = p // 2

        @pl.loop(0, N_EXP)
        def _(e):
            @pl.when((has[own * N_EXP + e] == 0) & (opts[e] > 1))
            def _():
                for a in range(N_CHIP):
                    for b in range(a + 1, N_CHIP):
                        both = (has[a * N_EXP + e] > 0) & (has[b * N_EXP + e] > 0)

                        @pl.when(both)
                        def _(a=a, b=b):
                            ka = chip_k[p * N_CHIP + a]
                            kb = chip_k[p * N_CHIP + b]
                            xa = x[X(p, a, e)]
                            xb = x[X(p, b, e)]
                            shift = lax.shift_right_arithmetic(ka - kb, i32(1))
                            shift = jnp.minimum(jnp.maximum(shift, -xb), xa)
                            x[X(p, a, e)] = xa - shift
                            x[X(p, b, e)] = xb + shift
                            chip_k[p * N_CHIP + a] = ka - shift
                            chip_k[p * N_CHIP + b] = kb + shift

    def worst(i, acc):
        p = i // N_CHIP
        away = p // 2 != i % N_CHIP
        return jnp.maximum(acc, jnp.where(away, chip_k[i], 0))

    top = lax.fori_loop(0, N_DEV * N_CHIP, worst, i32(0))
    pick = i32(0)
    for g in CAP_GRPS[:-1]:
        pick = pick + (top > 2 * g).astype(i32)
    pick_ref[0] = pick

    @pl.when(pick == len(CAP_GRPS) - 1)
    def _():
        @pl.loop(0, N_DEV * N_EXP)
        def _(i):
            p = i // N_EXP
            e = i % N_EXP
            g = grp[i]
            n = opts[e]
            done = i32(0)
            share = i32(0)
            for c in range(N_CHIP):
                done = done + has[c * N_EXP + e]
                upto = (g * done) // n
                x[X(p, c, e)] = upto - share
                share = upto

        chip_sums()

    def half(k):
        return (k + 1) // 2

    @pl.loop(0, N_EXP)
    def _(e):
        def before(c):
            def add(f, acc):
                return acc + jnp.where(f < e, x[X(me, c, f)], 0)
            return lax.fori_loop(0, N_EXP, add, i32(0))

        row = i32(0)
        prev = i32(0)

        def put(i, at, to):
            piece_at[i * N_EXP + e] = at * GROUP
            piece_add[i * N_EXP + e] = to - at * GROUP

        put(0, i32(0), before(chip) * GROUP)
        row = x[X(me, chip, e)]
        for step in range(1, N_CHIP):
            c = chip ^ step
            amt = x[X(me, c, e)]
            off = before(c)
            h0 = half(chip_k[me * N_CHIP + c])
            n0 = jnp.minimum(jnp.maximum(h0 - off, 0), amt)
            d0 = (2 * c) ^ me
            d1 = (2 * c + 1) ^ me
            put(2 * step - 1, row, cls_ref[d0] * AID * GROUP + off * GROUP)
            put(2 * step, row + n0, cls_ref[d1] * AID * GROUP + (off + n0 - h0) * GROUP)
            row = row + amt

    def expert_of(u):
        dev = me ^ (u // N_SLOT)
        return slot_ref[dev * N_SLOT + u % N_SLOT]

    def fresh_unit(u):
        e = expert_of(u)
        ok = jnp.bool_(True)
        for v in range(u):
            ok = ok & (expert_of(v) != e)
        return e, ok

    def close(call, u, first, ptr):
        t0 = first // TILE_G
        t1 = (ptr + TILE_G - 1) // TILE_G

        @pl.loop(t0, t1)
        def _(t):
            units[call][t] = i32(u)
            cnts[call][t] = jnp.minimum(ptr - t * TILE_G, TILE_G)

        return t1 * TILE_G

    for call in range(2):
        ptr = i32(0)
        for u in (2 * call, 2 * call + 1):
            e, ok = fresh_unit(u)

            def before(f, acc, e=e):
                return acc + jnp.where(f < e, x[X(me, chip, f)], 0)

            base = lax.fori_loop(0, N_EXP, before, i32(0))
            n = jnp.where(ok, x[X(me, chip, e)], 0)

            @pl.loop(0, n)
            def _(m, ptr=ptr, base=base, call=call):
                ents[call][ptr + m] = base + m

            ptr = close(call, u, ptr, ptr + n)
        nts[call][0] = ptr // TILE_G

    for b, classes in enumerate(BATCHES):
        call = 2 + b
        ptr = i32(0)
        for u in range(2 * N_SLOT):
            e, ok = fresh_unit(u)
            first = ptr
            for aid, ci in enumerate(classes):
                p = me ^ CLASSES[ci]

                def before(f, acc, e=e, p=p):
                    return acc + jnp.where(f < e, x[X(p, chip, f)], 0)

                beg = lax.fori_loop(0, N_EXP, before, i32(0))
                end = beg + x[X(p, chip, e)]
                k = chip_k[p * N_CHIP + chip]
                lo = jnp.where(core == 0, 0, half(k))
                hi = jnp.where(core == 0, half(k), k)
                beg = jnp.maximum(beg, lo)
                n = jnp.where(ok, jnp.maximum(jnp.minimum(end, hi) - beg, 0), 0)

                @pl.loop(0, n)
                def _(m, ptr=ptr, beg=beg, lo=lo, aid=aid, call=call):
                    ents[call][ptr + m] = beg - lo + m + aid * AID

                ptr = ptr + n
            ptr = close(call, u, first, ptr)
        nts[call][0] = ptr // TILE_G


def make_plan(counts, slot_expert, me):
    smem = pl.BlockSpec(memory_space=pltpu.SMEM)
    vec = lambda n: jax.ShapeDtypeStruct((n,), jnp.int32)
    s = lambda n: pltpu.SMEM((n,), jnp.int32)
    cls = jnp.array([1 + CLASSES.index(d) if d in CLASSES else 0 for d in range(N_DEV)], jnp.int32)
    outs = [vec(N_PIECE * N_EXP)] * 2 + [vec(1)] + [vec(MAX_E)] * N_CALL + [vec(MAX_T)] * (2 * N_CALL) + [vec(1)] * N_CALL
    res = pl.pallas_call(
        plan_kernel,
        out_shape=outs,
        in_specs=[smem] * 4,
        out_specs=[smem] * len(outs),
        scratch_shapes=[s(64), s(32), s(8), s(32), s(256)],
        name='plan',
    )(me.reshape(1), counts.reshape(-1), slot_expert.reshape(-1), cls)
    tabs = [[res[3 + k * N_CALL + i] for k in range(4)] for i in range(N_CALL)]
    return res[0], res[1], res[2], tabs


def ffn_kernel(ent, unit, cnt, nt_ref, idx, *refs, n_src, n_pair, by_row):
    srcs, refs = refs[:n_src], refs[n_src:]
    pairs, refs = refs[:2 * n_pair], refs[2 * n_pair:]
    if by_row:
        refs = refs[1:]
    outs, refs = refs[:n_src], refs[n_src:]
    xbuf, xt, obuf, ubuf, dbuf, acc, xsem, osem, wsem = refs
    nt = nt_ref[0]
    nf = pairs[0].shape[3] // TILE_F

    def weight_copies(s, fn):
        t = s // nf
        f = pl.multiple_of((s - t * nf) * TILE_F, TILE_F)
        b = s % 2
        u = unit[t]
        slot = u % N_SLOT
        for w in range(n_pair):
            def go(w=w):
                fn(pltpu.make_async_copy(pairs[2 * w].at[0, slot, :, pl.ds(f, TILE_F)], ubuf.at[b], wsem.at[b, 0]))
                fn(pltpu.make_async_copy(pairs[2 * w + 1].at[0, slot, pl.ds(f, TILE_F), :], dbuf.at[b], wsem.at[b, 1]))
            if n_pair == 1:
                go()
            else:
                pl.when(u // N_SLOT == w)(go)

    def x_start(t):
        b = t % 2

        @pl.loop(0, cnt[t])
        def _(m):
            v = ent[t * TILE_G + m]
            if by_row:
                for r in range(GROUP):
                    pltpu.make_async_copy(srcs[0].at[idx[v * GROUP + r]], xbuf.at[b, m * GROUP + r], xsem.at[b]).start()
            else:
                for a in range(n_src):
                    @pl.when(v // AID == a)
                    def _(a=a):
                        pltpu.make_async_copy(srcs[a].at[pl.ds((v % AID) * GROUP, GROUP)], xbuf.at[b, pl.ds(m * GROUP, GROUP)], xsem.at[b]).start()

    def x_wait(t):
        b = t % 2

        @pl.loop(0, cnt[t])
        def _(m):
            pltpu.make_async_copy(srcs[0].at[pl.ds(0, GROUP)], xbuf.at[b, pl.ds(0, GROUP)], xsem.at[b]).wait()

    def o_start(t):
        b = t % 2

        @pl.loop(0, cnt[t])
        def _(m):
            v = ent[t * TILE_G + m]
            for a in range(n_src):
                @pl.when(v // AID == a)
                def _(a=a):
                    pltpu.make_async_copy(obuf.at[b, pl.ds(m * GROUP, GROUP)], outs[a].at[pl.ds((v % AID) * GROUP, GROUP)], osem.at[b]).start()

    def o_wait(t):
        b = t % 2

        @pl.loop(0, cnt[t])
        def _(m):
            pltpu.make_async_copy(obuf.at[b, pl.ds(0, GROUP)], outs[0].at[pl.ds(0, GROUP)], osem.at[b]).wait()

    @pl.when(nt > 0)
    def _():
        weight_copies(0, lambda c: c.start())
        x_start(0)

    @pl.loop(0, nt)
    def _(i):
        x_wait(i)
        xt[...] = xbuf[i % 2].reshape(xt.shape)
        acc[...] = jnp.zeros_like(acc)

        @pl.when(i + 1 < nt)
        def _():
            x_start(i + 1)

        @pl.when(i >= 1)
        def _():
            o_start(i - 1)

        rows = cnt[i] * GROUP

        @pl.loop(0, nf)
        def _(j):
            step = i * nf + j

            @pl.when(step + 1 < nt * nf)
            def _():
                weight_copies(step + 1, lambda c: c.start())

            weight_copies(step, lambda c: c.wait())
            b = step % 2

            def run(m):
                pre = jnp.dot(xt[:m, :], ubuf[b], preferred_element_type=jnp.float32)
                hid = jax.nn.gelu(pre, approximate=True).astype(jnp.bfloat16)
                acc[:m, :] += jnp.dot(hid, dbuf[b], preferred_element_type=jnp.float32)

            pl.when(rows <= 128)(lambda: run(128))
            pl.when((rows > 128) & (rows <= 256))(lambda: run(256))
            pl.when(rows > 256)(lambda: run(TILE_M))

        @pl.when(i >= 2)
        def _():
            o_wait(i - 2)

        obuf[i % 2] = acc[...].astype(jnp.bfloat16).reshape(obuf.shape[1:])

    @pl.when(nt >= 1)
    def _():
        o_start(nt - 1)

        @pl.when(nt >= 2)
        def _():
            o_wait(nt - 2)

        o_wait(nt - 1)


def ffn(tab, idx, srcs, pairs, back, name):
    by_row = back is not None
    ent, unit, cnt, nt = tab
    flat = [w for pair in pairs for w in pair]
    d = flat[0].shape[2]
    f = flat[0].shape[3]
    any_spec = pl.BlockSpec(memory_space=pl.ANY)
    n_src = len(srcs)
    extra = [back] if by_row else []
    shapes = [jax.ShapeDtypeStruct(a.shape, a.dtype) for a in ([back] if by_row else srcs)]
    row = (d // LANE, LANE)
    rows_est = 2048
    smem = pl.BlockSpec(memory_space=pltpu.SMEM)
    return pl.pallas_call(
        functools.partial(ffn_kernel, n_src=n_src, n_pair=len(pairs), by_row=by_row),
        in_specs=[smem] * 5 + [any_spec] * (n_src + len(flat) + len(extra)),
        out_specs=[any_spec] * n_src,
        scratch_shapes=[
            pltpu.VMEM((2, TILE_M) + row, jnp.bfloat16),
            pltpu.VMEM((TILE_M, d), jnp.bfloat16),
            pltpu.VMEM((2, TILE_M) + row, jnp.bfloat16),
            pltpu.VMEM((2, d, TILE_F), jnp.bfloat16),
            pltpu.VMEM((2, TILE_F, d), jnp.bfloat16),
            pltpu.VMEM((TILE_M, d), jnp.float32),
            pltpu.SemaphoreType.DMA((2,)),
            pltpu.SemaphoreType.DMA((2,)),
            pltpu.SemaphoreType.DMA((2, 2)),
        ],
        out_shape=shapes,
        input_output_aliases={5 + n_src + len(flat): 0} if by_row else {},
        compiler_params=pltpu.CompilerParams(vmem_limit_bytes=VMEM_BYTES),
        cost_estimate=pl.CostEstimate(flops=4 * rows_est * d * f, bytes_accessed=100_000_000, transcendentals=rows_est * f),
        name=name,
    )(ent, unit, cnt, nt, idx, *srcs, *flat, *extra)


def pick_kernel(idx, src, o_ref, buf, sem):
    t = pl.program_id(0)
    n = pl.num_programs(0)
    rows = o_ref.shape[0]

    def start(k):
        @pl.loop(0, rows // 8)
        def _(m):
            for r in range(8):
                q = m * 8 + r
                pltpu.make_async_copy(src.at[idx[k * rows + q]], buf.at[k % 2, q], sem.at[k % 2]).start()

    pl.when(t == 0)(lambda: start(t))
    pl.when(t + 1 < n)(lambda: start(t + 1))
    pltpu.make_async_copy(src.at[pl.ds(0, rows)], buf.at[t % 2], sem.at[t % 2]).wait()
    o_ref[...] = buf[t % 2]


def pick_rows(src, idx, name):
    row = src.shape[1:]
    n = idx.shape[0]
    tile = n // 2
    return pl.pallas_call(
        pick_kernel,
        grid_spec=pltpu.PrefetchScalarGridSpec(
            num_scalar_prefetch=1,
            grid=(2,),
            in_specs=[pl.BlockSpec(memory_space=pl.ANY)],
            out_specs=pl.BlockSpec((tile,) + row, lambda t, s: (t, 0, 0)),
            scratch_shapes=[pltpu.VMEM((2, tile) + row, src.dtype), pltpu.SemaphoreType.DMA((2,))],
        ),
        out_shape=jax.ShapeDtypeStruct((n,) + row, src.dtype),
        compiler_params=pltpu.CompilerParams(vmem_limit_bytes=VMEM_BYTES),
        name=name,
    )(idx, src)


def mix_kernel(p0, p1, src, w0, w1, o_ref, buf, sem):
    t = pl.program_id(0)
    n = pl.num_programs(0)
    rows = o_ref.shape[0]

    def start(k):
        @pl.loop(0, rows // 4)
        def _(m):
            for r in range(4):
                q = m * 4 + r
                pltpu.make_async_copy(src.at[p0[k * rows + q]], buf.at[k % 2, 0, q], sem.at[k % 2, 0]).start()
                pltpu.make_async_copy(src.at[p1[k * rows + q]], buf.at[k % 2, 1, q], sem.at[k % 2, 1]).start()

    pl.when(t == 0)(lambda: start(t))
    pl.when(t + 1 < n)(lambda: start(t + 1))
    for h in range(2):
        pltpu.make_async_copy(src.at[pl.ds(0, rows)], buf.at[t % 2, h], sem.at[t % 2, h]).wait()
    y = buf[t % 2, 0].astype(jnp.float32) * w0[...] + buf[t % 2, 1].astype(jnp.float32) * w1[...]
    o_ref[...] = y.astype(o_ref.dtype).reshape(o_ref.shape)


def mix(back, pos, topk_w):
    row = back.shape[1:]
    n = pos[0].shape[0]
    d = row[0] * row[1]
    tile = 256
    wide = [jnp.broadcast_to(topk_w[:, k][:, None, None], (n, 1, LANE)) for k in range(2)]
    w_spec = pl.BlockSpec((tile, 1, LANE), lambda t, a, b: (t, 0, 0))
    return pl.pallas_call(
        mix_kernel,
        grid_spec=pltpu.PrefetchScalarGridSpec(
            num_scalar_prefetch=2,
            grid=(n // tile,),
            in_specs=[pl.BlockSpec(memory_space=pl.ANY), w_spec, w_spec],
            out_specs=pl.BlockSpec((tile, d), lambda t, a, b: (t, 0)),
            scratch_shapes=[pltpu.VMEM((2, 2, tile) + row, back.dtype), pltpu.SemaphoreType.DMA((2, 2))],
        ),
        out_shape=jax.ShapeDtypeStruct((n, d), back.dtype),
        compiler_params=pltpu.CompilerParams(vmem_limit_bytes=VMEM_BYTES),
        name='mix',
    )(pos[0], pos[1], back, *wide)


def fresh(shape):
    return pl.pallas_call(lambda o: None, out_shape=jax.ShapeDtypeStruct(shape, jnp.bfloat16), out_specs=pl.BlockSpec(memory_space=pl.ANY), name='fresh')()


def count_pairs(topk_idx):
    experts = jnp.arange(N_EXP, dtype=jnp.int32)
    hits = [topk_idx[:, j][None, :] == experts[:, None] for j in range(topk_idx.shape[1])]
    one = sum(h.astype(jnp.int32) for h in hits)
    incl = jnp.cumsum(one, axis=1)
    return hits, incl - one, incl[:, -1]


def invert(pos, n_rows):
    n_tok = pos[0].shape[0]
    lo_n = 64
    hi_ids = jnp.arange(n_rows // lo_n, dtype=jnp.int32)
    lo_ids = jnp.arange(2 * lo_n, dtype=jnp.int32)
    tok = jnp.arange(n_tok, dtype=jnp.int32)
    val = jnp.where(lo_ids[None, :] < lo_n, (tok // lo_n)[:, None], (tok % lo_n)[:, None])
    packed = 0.0
    for p in pos:
        left = ((p // lo_n)[None, :] == hi_ids[:, None]).astype(jnp.bfloat16)
        right = jnp.where((p % lo_n)[:, None] == (lo_ids % lo_n)[None, :], val, 0).astype(jnp.bfloat16)
        packed = packed + jnp.dot(left, right, preferred_element_type=jnp.float32)
    packed = packed.astype(jnp.int32)
    return (packed[:, :lo_n] * lo_n + packed[:, lo_n:]).reshape(-1)


def swap(a, d):
    return lax.ppermute(a, 'ep', [(p, p ^ d) for p in range(N_DEV)])


def layer_branch(cap_grps, tok3, pos_virtual, topk_w, w_up, w_down, tabs):
    cap = cap_grps * GROUP
    local = LOCAL_GRPS * GROUP
    row = tok3.shape[1:]
    n_cls = len(CLASSES)
    span = AID * GROUP
    pos = []
    for v in pos_virtual:
        ci = v // span
        pos.append(jnp.where(ci == 0, v, local + (ci - 1) * cap + v % span))
    total = local + n_cls * cap
    idx = invert(pos, (total + 63) // 64 * 64)
    sib = (swap(w_up, 1), swap(w_down, 1))
    own = (w_up, w_down)
    sent = []
    for ci, d in enumerate(CLASSES):
        lo = local + ci * cap
        sent.append(swap(pick_rows(tok3, idx[lo:lo + cap], f'pick{ci}'), d))
    loc_idx = idx[:local]
    back = fresh((total,) + row)
    (back,) = ffn(tabs[0], loc_idx, [tok3], [own], back, 'ffn_own')
    home = [None] * n_cls
    for b, classes in enumerate(BATCHES):
        outs = ffn(tabs[2 + b], loc_idx[:8], [sent[ci] for ci in classes], [own, sib], None, f'ffn_b{b}')
        for ci, o in zip(classes, outs):
            home[ci] = swap(o, CLASSES[ci])
    (back,) = ffn(tabs[1], loc_idx, [tok3], [sib], back, 'ffn_sib')
    for ci in range(n_cls):
        back = lax.dynamic_update_slice(back, home[ci], (local + ci * cap, 0, 0))
    return mix(back, pos, topk_w)


def solution(mesh):
    def group_layer(tokens, topk_idx, topk_w, w_up, w_down, slot_expert):
        n_tok, d = tokens.shape
        me = lax.axis_index('ep').astype(jnp.int32)
        hits, rank, counts = count_pairs(topk_idx)
        all_counts = lax.all_gather(counts, 'ep')
        at, add, pick, tabs = make_plan(all_counts, slot_expert, me)
        at = at.reshape(N_PIECE, N_EXP, 1)
        add = add.reshape(N_PIECE, N_EXP, 1)
        place = rank + add[0]
        for i in range(1, N_PIECE):
            place = jnp.where(rank >= at[i], rank + add[i], place)
        pos = [jnp.sum(jnp.where(h, place, 0), axis=0) for h in hits]
        tok3 = tokens.reshape(n_tok, d // LANE, LANE)
        branches = [functools.partial(layer_branch, g) for g in CAP_GRPS]
        return lax.switch(pick[0], branches, tok3, pos, topk_w, w_up, w_down, tabs)

    row_spec = P(('dp', 'ep'), None)
    weight_spec = P('ep', None, None, None)
    return jax.shard_map(group_layer, mesh=mesh, in_specs=(row_spec, row_spec, row_spec, weight_spec, weight_spec, P(None, None)), out_specs=row_spec, check_vma=False)
```

```python
import functools

import jax
import jax.numpy as jnp
from jax import lax
from jax.experimental import pallas as pl
from jax.experimental.pallas import tpu as pltpu
from jax.sharding import PartitionSpec as P


GROUP = 16
N_DEV = 8
N_CHIP = 4
N_SLOT = 2
N_EXP = 8
N_UNIT = N_DEV * N_SLOT
N_PIECE = 7
TILE_G = 32
TILE_M = TILE_G * GROUP
TILE_F = 512
SWEEPS = 3
SIZES = (256, 384, 512)
LANE = 128
CLASSES = (2, 4, 6, 7, 3, 5)
BATCHES = ((0, 1, 2), (3, 4, 5))
PICKS = ((0, 1), (2, 3, 4, 5))
GOALS = (250, 390)
TILE_COST = 16
ROW_COST = 17
CAP_GRPS = (49, 58, 98)
LOCAL_GRPS = 520
MAX_T = 20
MAX_E = MAX_T * TILE_G
N_CALL = 1 + len(BATCHES)
N_RANGE = 1 + 2 * len(BATCHES)
AID = 4096
DEPTH = 3
GELU_A = 0.7978845608
GELU_B = GELU_A * 0.044715
VMEM_BYTES = 60 * 1024 * 1024


def plan_kernel(me_ref, cnt_ref, slot_ref, cls_ref, piece_at, piece_add, pick_ref, *refs):
    ents, units, cnts = (refs[i * N_CALL:(i + 1) * N_CALL] for i in range(3))
    ranges = refs[3 * N_CALL:3 * N_CALL + N_RANGE]
    grp, has, opts, chip_k, loads, x = refs[3 * N_CALL + N_RANGE:]
    i32 = jnp.int32
    me = me_ref[0]
    chip = me // 2
    core = me % 2

    def X(p, c, e):
        return (p * N_CHIP + c) * N_EXP + e

    @pl.loop(0, N_CHIP * N_EXP)
    def _(i):
        has[i] = i32(0)

    @pl.loop(0, N_EXP)
    def _(i):
        opts[i] = i32(0)

    @pl.loop(0, N_UNIT)
    def _(k):
        e = slot_ref[k]
        i = (k // 4) * N_EXP + e
        has[i] = has[i] + 1
        opts[e] = opts[e] + 1

    @pl.loop(0, N_DEV * N_EXP)
    def _(i):
        g = (cnt_ref[i] + (GROUP - 1)) // GROUP
        grp[i] = g
        p = i // N_EXP
        e = i % N_EXP
        own = p // 2
        at_home = has[own * N_EXP + e] > 0
        left = g
        for c in range(N_CHIP):
            here = jnp.where(at_home, own == c, has[c * N_EXP + e] > 0)
            amt = jnp.where(here, left, 0)
            x[X(p, c, e)] = amt
            left = left - amt

    def chip_sums():
        @pl.loop(0, N_DEV * N_CHIP)
        def _(i):
            def add(e, acc):
                return acc + x[i * N_EXP + e]
            chip_k[i] = lax.fori_loop(0, N_EXP, add, i32(0))

    chip_sums()

    @pl.loop(0, N_DEV * SWEEPS)
    def _(i):
        p = i // SWEEPS
        own = p // 2

        @pl.loop(0, N_EXP)
        def _(e):
            @pl.when((has[own * N_EXP + e] == 0) & (opts[e] > 1))
            def _():
                for a in range(N_CHIP):
                    for b in range(a + 1, N_CHIP):
                        both = (has[a * N_EXP + e] > 0) & (has[b * N_EXP + e] > 0)

                        @pl.when(both)
                        def _(a=a, b=b):
                            ka = chip_k[p * N_CHIP + a]
                            kb = chip_k[p * N_CHIP + b]
                            xa = x[X(p, a, e)]
                            xb = x[X(p, b, e)]
                            shift = lax.shift_right_arithmetic(ka - kb, i32(1))
                            shift = jnp.minimum(jnp.maximum(shift, -xb), xa)
                            x[X(p, a, e)] = xa - shift
                            x[X(p, b, e)] = xb + shift
                            chip_k[p * N_CHIP + a] = ka - shift
                            chip_k[p * N_CHIP + b] = kb + shift

    def worst(i, acc):
        p = i // N_CHIP
        away = p // 2 != i % N_CHIP
        return jnp.maximum(acc, jnp.where(away, chip_k[i], 0))

    top = lax.fori_loop(0, N_DEV * N_CHIP, worst, i32(0))
    pick = i32(0)
    for g in CAP_GRPS[:-1]:
        pick = pick + (top > 2 * g).astype(i32)
    pick_ref[0] = pick

    @pl.when(pick < len(CAP_GRPS) - 1)
    def _():
        room = i32(0)
        for i, g in enumerate(CAP_GRPS[:-1]):
            room = jnp.where(pick == i, 2 * g, room)
        for c in range(N_CHIP):
            def add(p, acc, c=c):
                return acc + chip_k[p * N_CHIP + c]
            loads[c] = lax.fori_loop(0, N_DEV, add, i32(0))

        @pl.loop(0, N_DEV)
        def _(p):
            own = p // 2

            @pl.loop(0, N_EXP)
            def _(e):
                @pl.when(opts[e] > 1)
                def _():
                    for a in range(N_CHIP):
                        for b in range(a + 1, N_CHIP):
                            both = (has[a * N_EXP + e] > 0) & (has[b * N_EXP + e] > 0)

                            @pl.when(both)
                            def _(a=a, b=b):
                                ka = chip_k[p * N_CHIP + a]
                                kb = chip_k[p * N_CHIP + b]
                                xa = x[X(p, a, e)]
                                xb = x[X(p, b, e)]
                                free_a = jnp.where(own == a, AID, room - ka)
                                free_b = jnp.where(own == b, AID, room - kb)
                                shift = lax.shift_right_arithmetic(loads[a] - loads[b], i32(1))
                                shift = jnp.minimum(shift, jnp.minimum(xa, free_b))
                                shift = jnp.maximum(shift, -jnp.minimum(xb, free_a))
                                x[X(p, a, e)] = xa - shift
                                x[X(p, b, e)] = xb + shift
                                chip_k[p * N_CHIP + a] = ka - shift
                                chip_k[p * N_CHIP + b] = kb + shift
                                loads[a] = loads[a] - shift
                                loads[b] = loads[b] + shift

    @pl.when(pick == len(CAP_GRPS) - 1)
    def _():
        @pl.loop(0, N_DEV * N_EXP)
        def _(i):
            p = i // N_EXP
            e = i % N_EXP
            g = grp[i]
            n = opts[e]
            done = i32(0)
            share = i32(0)
            for c in range(N_CHIP):
                done = done + has[c * N_EXP + e]
                upto = (g * done) // n
                x[X(p, c, e)] = upto - share
                share = upto

        chip_sums()

    def half(k):
        return (k + 1) // 2

    @pl.loop(0, N_EXP)
    def _(e):
        def before(c):
            def add(f, acc):
                return acc + jnp.where(f < e, x[X(me, c, f)], 0)
            return lax.fori_loop(0, N_EXP, add, i32(0))

        row = i32(0)
        prev = i32(0)

        def put(i, at, to):
            piece_at[i * N_EXP + e] = at * GROUP
            piece_add[i * N_EXP + e] = to - at * GROUP

        put(0, i32(0), before(chip) * GROUP)
        row = x[X(me, chip, e)]
        for step in range(1, N_CHIP):
            c = chip ^ step
            amt = x[X(me, c, e)]
            off = before(c)
            h0 = half(chip_k[me * N_CHIP + c])
            n0 = jnp.minimum(jnp.maximum(h0 - off, 0), amt)
            d0 = (2 * c) ^ me
            d1 = (2 * c + 1) ^ me
            put(2 * step - 1, row, cls_ref[d0] * AID * GROUP + off * GROUP)
            put(2 * step, row + n0, cls_ref[d1] * AID * GROUP + (off + n0 - h0) * GROUP)
            row = row + amt

    def expert_of(u):
        dev = me ^ (u // N_SLOT)
        return slot_ref[dev * N_SLOT + u % N_SLOT]

    def fresh_unit(u):
        e = expert_of(u)
        ok = jnp.bool_(True)
        for v in range(u):
            ok = ok & (expert_of(v) != e)
        return e, ok

    def close(call, u, first, ptr):
        t0 = first // TILE_G
        t1 = (ptr + TILE_G - 1) // TILE_G

        @pl.loop(t0, t1)
        def _(t):
            units[call][t] = i32(u)
            cnts[call][t] = jnp.minimum(ptr - t * TILE_G, TILE_G)

        return t1 * TILE_G

    ptr = i32(0)
    own_tiles = i32(0)
    for u in range(2 * N_SLOT):
        e, ok = fresh_unit(u)

        def before(f, acc, e=e):
            return acc + jnp.where(f < e, x[X(me, chip, f)], 0)

        base = lax.fori_loop(0, N_EXP, before, i32(0))
        n = jnp.where(ok, x[X(me, chip, e)], 0)

        @pl.loop(0, n)
        def _(m, ptr=ptr, base=base):
            ents[0][ptr + m] = base + m

        ptr = close(0, u, ptr, ptr + n)
        if u == N_SLOT - 1:
            own_tiles = ptr // TILE_G
    all_tiles = ptr // TILE_G

    for b, classes in enumerate(BATCHES):
        call = 1 + b
        ptr = i32(0)
        for u in range(2 * N_SLOT):
            e, ok = fresh_unit(u)
            first = ptr
            for aid, ci in enumerate(classes):
                p = me ^ CLASSES[ci]

                def before(f, acc, e=e, p=p):
                    return acc + jnp.where(f < e, x[X(p, chip, f)], 0)

                beg = lax.fori_loop(0, N_EXP, before, i32(0))
                end = beg + x[X(p, chip, e)]
                k = chip_k[p * N_CHIP + chip]
                lo = jnp.where(core == 0, 0, half(k))
                hi = jnp.where(core == 0, half(k), k)
                beg = jnp.maximum(beg, lo)
                n = jnp.where(ok, jnp.maximum(jnp.minimum(end, hi) - beg, 0), 0)

                @pl.loop(0, n)
                def _(m, ptr=ptr, beg=beg, lo=lo, aid=aid, call=call):
                    ents[call][ptr + m] = beg - lo + m + aid * AID

                ptr = ptr + n
            ptr = close(call, u, first, ptr)
        ranges[2 * b + 1][0] = i32(0)
        ranges[2 * b + 1][1] = ptr // TILE_G

    def cost(call, t):
        return TILE_COST + (cnts[call][t] * ROW_COST) // TILE_G

    done = i32(0)
    spent = i32(0)
    for b, goal in enumerate(GOALS):
        def add(t, acc, b=b):
            return acc + cost(1 + b, t)

        batch = lax.fori_loop(0, ranges[2 * b + 1][1], add, i32(0))
        limit = own_tiles if b == 0 else all_tiles

        def fill(t, carry, room=goal - batch):
            upto, used = carry
            more = used < room
            return upto + more.astype(i32), used + jnp.where(more, cost(0, t), 0)

        upto, spent = lax.fori_loop(done, jnp.maximum(limit, done), fill, (done, spent))
        ranges[2 * b][0] = done
        ranges[2 * b][1] = upto
        done = upto
        spent = spent + batch
    ranges[N_RANGE - 1][0] = done
    ranges[N_RANGE - 1][1] = all_tiles


def make_plan(counts, slot_expert, me):
    smem = pl.BlockSpec(memory_space=pltpu.SMEM)
    vec = lambda n: jax.ShapeDtypeStruct((n,), jnp.int32)
    s = lambda n: pltpu.SMEM((n,), jnp.int32)
    cls = jnp.array([1 + CLASSES.index(d) if d in CLASSES else 0 for d in range(N_DEV)], jnp.int32)
    outs = [vec(N_PIECE * N_EXP)] * 2 + [vec(1)] + [vec(MAX_E)] * N_CALL + [vec(MAX_T)] * (2 * N_CALL) + [vec(2)] * N_RANGE
    res = pl.pallas_call(
        plan_kernel,
        out_shape=outs,
        in_specs=[smem] * 4,
        out_specs=[smem] * len(outs),
        scratch_shapes=[s(64), s(32), s(8), s(32), s(8), s(256)],
        name='plan',
    )(me.reshape(1), counts.reshape(-1), slot_expert.reshape(-1), cls)
    tabs = [[res[3 + k * N_CALL + i] for k in range(3)] for i in range(N_CALL)]
    return res[0], res[1], res[2], tabs, res[3 + 3 * N_CALL:]


def ffn_kernel(ent, unit, cnt, span, idx, *refs, n_src, n_pair, by_row):
    srcs, refs = refs[:n_src], refs[n_src:]
    pairs, refs = refs[:2 * n_pair], refs[2 * n_pair:]
    if by_row:
        refs = refs[1:]
    outs, refs = refs[:n_src], refs[n_src:]
    xbuf, xt, obuf, ubuf, dbuf, acc, xsem, osem, wsem = refs
    first = span[0]
    nt = span[1] - first
    nf = pairs[0].shape[3] // TILE_F
    depth = ubuf.shape[0]

    def weight_copies(s, fn):
        k = s // nf
        f = pl.multiple_of((s - k * nf) * TILE_F, TILE_F)
        b = s % depth
        u = unit[first + k]
        slot = u % N_SLOT
        for w in range(n_pair):
            def go(w=w):
                fn(pltpu.make_async_copy(pairs[2 * w].at[0, slot, :, pl.ds(f, TILE_F)], ubuf.at[b], wsem.at[b, 0]))
                fn(pltpu.make_async_copy(pairs[2 * w + 1].at[0, slot, pl.ds(f, TILE_F), :], dbuf.at[b], wsem.at[b, 1]))
            if n_pair == 1:
                go()
            else:
                pl.when(u // N_SLOT == w)(go)

    def weights_wait(s):
        b = s % depth
        pltpu.make_async_copy(pairs[0].at[0, 0, :, pl.ds(0, TILE_F)], ubuf.at[b], wsem.at[b, 0]).wait()
        pltpu.make_async_copy(pairs[1].at[0, 0, pl.ds(0, TILE_F), :], dbuf.at[b], wsem.at[b, 1]).wait()

    def x_start(k):
        b = k % 2
        t = first + k

        @pl.loop(0, cnt[t])
        def _(m):
            v = ent[t * TILE_G + m]
            if by_row:
                for r in range(GROUP):
                    pltpu.make_async_copy(srcs[0].at[idx[v * GROUP + r]], xbuf.at[b, m * GROUP + r], xsem.at[b]).start()
            else:
                for a in range(n_src):
                    @pl.when(v // AID == a)
                    def _(a=a):
                        pltpu.make_async_copy(srcs[a].at[pl.ds((v % AID) * GROUP, GROUP)], xbuf.at[b, pl.ds(m * GROUP, GROUP)], xsem.at[b]).start()

    def x_wait(k):
        b = k % 2

        @pl.loop(0, cnt[first + k])
        def _(m):
            pltpu.make_async_copy(srcs[0].at[pl.ds(0, GROUP)], xbuf.at[b, pl.ds(0, GROUP)], xsem.at[b]).wait()

    def o_start(k):
        b = k % 2
        t = first + k

        @pl.loop(0, cnt[t])
        def _(m):
            v = ent[t * TILE_G + m]
            for a in range(n_src):
                @pl.when(v // AID == a)
                def _(a=a):
                    pltpu.make_async_copy(obuf.at[b, pl.ds(m * GROUP, GROUP)], outs[a].at[pl.ds((v % AID) * GROUP, GROUP)], osem.at[b]).start()

    def o_wait(k):
        b = k % 2

        @pl.loop(0, cnt[first + k])
        def _(m):
            pltpu.make_async_copy(obuf.at[b, pl.ds(0, GROUP)], outs[0].at[pl.ds(0, GROUP)], osem.at[b]).wait()

    @pl.when(nt > 0)
    def _():
        for s in range(depth - 1):
            weight_copies(s, lambda c: c.start())
        x_start(0)

    @pl.loop(0, nt)
    def _(k):
        x_wait(k)
        xt[...] = xbuf[k % 2].reshape(xt.shape)
        acc[...] = jnp.zeros_like(acc)

        @pl.when(k + 1 < nt)
        def _():
            x_start(k + 1)

        @pl.when(k >= 1)
        def _():
            o_start(k - 1)

        rows = cnt[first + k] * GROUP

        @pl.loop(0, nf)
        def _(j):
            s = k * nf + j
            weights_wait(s)

            @pl.when(s + depth - 1 < nt * nf)
            def _():
                weight_copies(s + depth - 1, lambda c: c.start())

            b = s % depth

            def run(m):
                pre = jnp.dot(xt[:m, :], ubuf[b], preferred_element_type=jnp.float32)
                bend = jnp.tanh(pre * (GELU_A + GELU_B * (pre * pre)))
                hid = (0.5 * pre * (1.0 + bend)).astype(jnp.bfloat16)
                acc[:m, :] += jnp.dot(hid, dbuf[b], preferred_element_type=jnp.float32)

            for m in SIZES:
                lo = max([v for v in SIZES if v < m], default=0)
                pl.when((rows > lo) & (rows <= m))(functools.partial(run, m))

        @pl.when(k >= 2)
        def _():
            o_wait(k - 2)

        obuf[k % 2] = acc[...].astype(jnp.bfloat16).reshape(obuf.shape[1:])

    @pl.when(nt >= 1)
    def _():
        @pl.when(nt >= 2)
        def _():
            o_wait(nt - 2)

        o_start(nt - 1)
        o_wait(nt - 1)


def ffn(tab, span, idx, srcs, pairs, back, name):
    by_row = back is not None
    ent, unit, cnt = tab
    flat = [w for pair in pairs for w in pair]
    d = flat[0].shape[2]
    f = flat[0].shape[3]
    any_spec = pl.BlockSpec(memory_space=pl.ANY)
    n_src = len(srcs)
    extra = [back] if by_row else []
    shapes = [jax.ShapeDtypeStruct(a.shape, a.dtype) for a in ([back] if by_row else srcs)]
    row = (d // LANE, LANE)
    rows_est = 2048
    smem = pl.BlockSpec(memory_space=pltpu.SMEM)
    return pl.pallas_call(
        functools.partial(ffn_kernel, n_src=n_src, n_pair=len(pairs), by_row=by_row),
        in_specs=[smem] * 5 + [any_spec] * (n_src + len(flat) + len(extra)),
        out_specs=[any_spec] * n_src,
        scratch_shapes=[
            pltpu.VMEM((2, TILE_M) + row, jnp.bfloat16),
            pltpu.VMEM((TILE_M, d), jnp.bfloat16),
            pltpu.VMEM((2, TILE_M) + row, jnp.bfloat16),
            pltpu.VMEM((DEPTH, d, TILE_F), jnp.bfloat16),
            pltpu.VMEM((DEPTH, TILE_F, d), jnp.bfloat16),
            pltpu.VMEM((TILE_M, d), jnp.float32),
            pltpu.SemaphoreType.DMA((2,)),
            pltpu.SemaphoreType.DMA((2,)),
            pltpu.SemaphoreType.DMA((DEPTH, 2)),
        ],
        out_shape=shapes,
        input_output_aliases={5 + n_src + len(flat): 0} if by_row else {},
        compiler_params=pltpu.CompilerParams(vmem_limit_bytes=VMEM_BYTES),
        cost_estimate=pl.CostEstimate(flops=4 * rows_est * d * f, bytes_accessed=100_000_000, transcendentals=rows_est * f),
        name=name,
    )(ent, unit, cnt, span, idx, *srcs, *flat, *extra)


def pick_kernel(idx, src, *refs, per):
    outs, (buf, sem) = refs[:-2], refs[-2:]
    t = pl.program_id(0)
    n = pl.num_programs(0)
    rows = outs[0].shape[0]

    def start(k):
        @pl.loop(0, rows // 8)
        def _(m):
            for r in range(8):
                q = m * 8 + r
                pltpu.make_async_copy(src.at[idx[k * rows + q]], buf.at[k % 2, q], sem.at[k % 2]).start()

    pl.when(t == 0)(lambda: start(t))
    pl.when(t + 1 < n)(lambda: start(t + 1))
    pltpu.make_async_copy(src.at[pl.ds(0, rows)], buf.at[t % 2], sem.at[t % 2]).wait()
    for c, o in enumerate(outs):
        @pl.when(t // per == c)
        def _(o=o):
            o[...] = buf[t % 2]


def pick_rows(src, idx, n_out, name):
    row = src.shape[1:]
    n = idx.shape[0] // n_out
    per = 2
    tile = n // per

    def spec(c):
        return pl.BlockSpec((tile,) + row, lambda t, s: (jnp.clip(t - c * per, 0, per - 1), 0, 0))

    return pl.pallas_call(
        functools.partial(pick_kernel, per=per),
        grid_spec=pltpu.PrefetchScalarGridSpec(
            num_scalar_prefetch=1,
            grid=(per * n_out,),
            in_specs=[pl.BlockSpec(memory_space=pl.ANY)],
            out_specs=[spec(c) for c in range(n_out)],
            scratch_shapes=[pltpu.VMEM((2, tile) + row, src.dtype), pltpu.SemaphoreType.DMA((2,))],
        ),
        out_shape=[jax.ShapeDtypeStruct((n,) + row, src.dtype)] * n_out,
        compiler_params=pltpu.CompilerParams(vmem_limit_bytes=VMEM_BYTES),
        name=name,
    )(idx, src)


def mix_kernel(p0, p1, src, w, o_ref, buf, sem):
    t = pl.program_id(0)
    n = pl.num_programs(0)
    rows = o_ref.shape[0]

    def start(k):
        @pl.loop(0, rows // 4)
        def _(m):
            for r in range(4):
                q = m * 4 + r
                pltpu.make_async_copy(src.at[p0[k * rows + q]], buf.at[k % 2, 0, q], sem.at[k % 2, 0]).start()
                pltpu.make_async_copy(src.at[p1[k * rows + q]], buf.at[k % 2, 1, q], sem.at[k % 2, 1]).start()

    pl.when(t == 0)(lambda: start(t))
    pl.when(t + 1 < n)(lambda: start(t + 1))
    for h in range(2):
        pltpu.make_async_copy(src.at[pl.ds(0, rows)], buf.at[t % 2, h], sem.at[t % 2, h]).wait()
    a, b = (buf[t % 2, h].reshape(o_ref.shape).astype(jnp.float32) for h in range(2))
    o_ref[...] = (a * w[:, :1] + b * w[:, 1:]).astype(o_ref.dtype)


def mix(back, pos, topk_w):
    row = back.shape[1:]
    n = pos[0].shape[0]
    d = row[0] * row[1]
    tile = 256
    w_spec = pl.BlockSpec((tile, topk_w.shape[1]), lambda t, a, b: (t, 0))
    return pl.pallas_call(
        mix_kernel,
        grid_spec=pltpu.PrefetchScalarGridSpec(
            num_scalar_prefetch=2,
            grid=(n // tile,),
            in_specs=[pl.BlockSpec(memory_space=pl.ANY), w_spec],
            out_specs=pl.BlockSpec((tile, d), lambda t, a, b: (t, 0)),
            scratch_shapes=[pltpu.VMEM((2, 2, tile) + row, back.dtype), pltpu.SemaphoreType.DMA((2, 2))],
        ),
        out_shape=jax.ShapeDtypeStruct((n, d), back.dtype),
        compiler_params=pltpu.CompilerParams(vmem_limit_bytes=VMEM_BYTES),
        name='mix',
    )(pos[0], pos[1], back, topk_w)


def fresh(shape):
    return pl.pallas_call(lambda o: None, out_shape=jax.ShapeDtypeStruct(shape, jnp.bfloat16), out_specs=pl.BlockSpec(memory_space=pl.ANY), name='fresh')()


def count_pairs(topk_idx):
    experts = jnp.arange(N_EXP, dtype=jnp.int32)
    hits = [topk_idx[:, j][None, :] == experts[:, None] for j in range(topk_idx.shape[1])]
    one = sum(h.astype(jnp.int32) for h in hits)
    incl = jnp.cumsum(one, axis=1)
    return hits, incl - one, incl[:, -1]


def invert(pos, n_rows):
    n_tok = pos[0].shape[0]
    lo_n = 64
    hi_ids = jnp.arange(n_rows // lo_n, dtype=jnp.int32)
    lo_ids = jnp.arange(2 * lo_n, dtype=jnp.int32)
    tok = jnp.arange(n_tok, dtype=jnp.int32)
    val = jnp.where(lo_ids[None, :] < lo_n, (tok // lo_n)[:, None] + 1, (tok % lo_n)[:, None])
    packed = 0.0
    for p in pos:
        left = ((p // lo_n)[None, :] == hi_ids[:, None]).astype(jnp.bfloat16)
        right = jnp.where((p % lo_n)[:, None] == (lo_ids % lo_n)[None, :], val, 0).astype(jnp.bfloat16)
        packed = packed + jnp.dot(left, right, preferred_element_type=jnp.float32)
    packed = packed.astype(jnp.int32)
    spare = (hi_ids[:, None] * lo_n + jnp.arange(lo_n, dtype=jnp.int32)[None, :]) % n_tok
    return jnp.where(packed[:, :lo_n] > 0, (packed[:, :lo_n] - 1) * lo_n + packed[:, lo_n:], spare).reshape(-1)


def swap(a, d):
    return lax.ppermute(a, 'ep', [(p, p ^ d) for p in range(N_DEV)])


def layer_branch(cap_grps, tok3, pos_virtual, topk_w, w_up, w_down, tabs, spans):
    cap = cap_grps * GROUP
    local = LOCAL_GRPS * GROUP
    row = tok3.shape[1:]
    n_cls = len(CLASSES)
    span = AID * GROUP
    pos = []
    for v in pos_virtual:
        ci = v // span
        pos.append(jnp.where(ci == 0, v, local + (ci - 1) * cap + v % span))
    total = local + n_cls * cap
    idx = invert(pos, (total + 63) // 64 * 64)
    own = (w_up, w_down)
    sent = []
    for classes in PICKS:
        lo = local + classes[0] * cap
        part = idx[lo:lo + len(classes) * cap]
        if sent:
            part, got[-1] = lax.optimization_barrier((part, got[-1]))
            sent[-1] = swap(got[-1], CLASSES[len(sent) - 1])
        got = list(pick_rows(tok3, part, len(classes), f'pick{classes[0]}'))
        sent += [swap(g, CLASSES[ci]) for g, ci in zip(got, classes)]
    up, down, _ = lax.optimization_barrier((w_up, w_down, got[-1]))
    sib = (swap(up, 1), swap(down, 1))
    loc_idx = idx[:local]
    back = fresh((total,) + row)
    home = [None] * n_cls
    for b, classes in enumerate(BATCHES):
        (back,) = ffn(tabs[0], spans[2 * b], loc_idx, [tok3], [own, sib][:1 + b], back, f'ffn_l{b}')
        outs = ffn(tabs[1 + b], spans[2 * b + 1], loc_idx[:8], [sent[ci] for ci in classes], [own, sib], None, f'ffn_b{b}')
        for ci, o in zip(classes, outs):
            home[ci] = swap(o, CLASSES[ci])
    (back,) = ffn(tabs[0], spans[-1], loc_idx, [tok3], [own, sib], back, 'ffn_end')
    for ci in range(n_cls):
        back = lax.dynamic_update_slice(back, home[ci], (local + ci * cap, 0, 0))
    return mix(back, pos, topk_w)


def solution(mesh):
    def group_layer(tokens, topk_idx, topk_w, w_up, w_down, slot_expert):
        n_tok, d = tokens.shape
        me = lax.axis_index('ep').astype(jnp.int32)
        hits, rank, counts = count_pairs(topk_idx)
        all_counts = lax.all_to_all(jnp.broadcast_to(counts, (N_DEV, N_EXP)), 'ep', 0, 0, tiled=True)
        tok3, all_counts = lax.optimization_barrier((tokens.reshape(n_tok, d // LANE, LANE), all_counts))
        at, add, pick, tabs, spans = make_plan(all_counts, slot_expert, me)
        at = at.reshape(N_PIECE, N_EXP, 1)
        add = add.reshape(N_PIECE, N_EXP, 1)
        place = rank + add[0]
        for i in range(1, N_PIECE):
            place = jnp.where(rank >= at[i], rank + add[i], place)
        pos = [jnp.sum(jnp.where(h, place, 0), axis=0) for h in hits]
        branches = [functools.partial(layer_branch, g) for g in CAP_GRPS]
        return lax.switch(pick[0], branches, tok3, pos, topk_w, w_up, w_down, tabs, spans)

    row_spec = P(('dp', 'ep'), None)
    weight_spec = P('ep', None, None, None)
    return jax.shard_map(group_layer, mesh=mesh, in_specs=(row_spec, row_spec, row_spec, weight_spec, weight_spec, P(None, None)), out_specs=row_spec, check_vma=False)
```

```python
import functools

import jax
import jax.numpy as jnp
from jax import lax
from jax.experimental import pallas as pl
from jax.experimental.pallas import tpu as pltpu
from jax.sharding import PartitionSpec as P


GROUP = 16
N_DEV = 8
N_CHIP = 4
N_SLOT = 2
N_EXP = 8
N_UNIT = N_DEV * N_SLOT
N_PIECE = 7
TILE_G = 32
TILE_M = TILE_G * GROUP
TILE_F = 512
SWEEPS = 3
SIZES = (256, 384, 512)
LANE = 128
CLASSES = (2, 4, 6, 7, 3, 5)
BATCHES = ((0, 1, 2), (3, 4, 5))
GOALS = (145, 420)
TILE_COST = 16
ROW_COST = 17
CAP_GRPS = (49, 58, 98)
LOCAL_GRPS = 520
MAX_T = 20
MAX_E = MAX_T * TILE_G
N_CALL = 1 + len(BATCHES)
N_RANGE = 1 + 2 * len(BATCHES)
AID = 4096
DEPTH = 3
GELU_A = 0.7978845608
GELU_B = GELU_A * 0.044715
VMEM_BYTES = 60 * 1024 * 1024


def plan_kernel(me_ref, cnt_ref, slot_ref, cls_ref, piece_at, piece_add, pick_ref, *refs):
    ents, units, cnts = (refs[i * N_CALL:(i + 1) * N_CALL] for i in range(3))
    ranges = refs[3 * N_CALL:3 * N_CALL + N_RANGE]
    grp, has, opts, chip_k, loads, x = refs[3 * N_CALL + N_RANGE:]
    i32 = jnp.int32
    me = me_ref[0]
    chip = me // 2
    core = me % 2

    def X(p, c, e):
        return (p * N_CHIP + c) * N_EXP + e

    @pl.loop(0, N_CHIP * N_EXP)
    def _(i):
        has[i] = i32(0)

    @pl.loop(0, N_EXP)
    def _(i):
        opts[i] = i32(0)

    @pl.loop(0, N_UNIT)
    def _(k):
        e = slot_ref[k]
        i = (k // 4) * N_EXP + e
        has[i] = has[i] + 1
        opts[e] = opts[e] + 1

    @pl.loop(0, N_DEV * N_EXP)
    def _(i):
        g = (cnt_ref[i] + (GROUP - 1)) // GROUP
        grp[i] = g
        p = i // N_EXP
        e = i % N_EXP
        own = p // 2
        at_home = has[own * N_EXP + e] > 0
        left = g
        for c in range(N_CHIP):
            here = jnp.where(at_home, own == c, has[c * N_EXP + e] > 0)
            amt = jnp.where(here, left, 0)
            x[X(p, c, e)] = amt
            left = left - amt

    def chip_sums():
        @pl.loop(0, N_DEV * N_CHIP)
        def _(i):
            def add(e, acc):
                return acc + x[i * N_EXP + e]
            chip_k[i] = lax.fori_loop(0, N_EXP, add, i32(0))

    chip_sums()

    @pl.loop(0, N_DEV * SWEEPS)
    def _(i):
        p = i // SWEEPS
        own = p // 2

        @pl.loop(0, N_EXP)
        def _(e):
            @pl.when((has[own * N_EXP + e] == 0) & (opts[e] > 1))
            def _():
                for a in range(N_CHIP):
                    for b in range(a + 1, N_CHIP):
                        both = (has[a * N_EXP + e] > 0) & (has[b * N_EXP + e] > 0)

                        @pl.when(both)
                        def _(a=a, b=b):
                            ka = chip_k[p * N_CHIP + a]
                            kb = chip_k[p * N_CHIP + b]
                            xa = x[X(p, a, e)]
                            xb = x[X(p, b, e)]
                            shift = lax.shift_right_arithmetic(ka - kb, i32(1))
                            shift = jnp.minimum(jnp.maximum(shift, -xb), xa)
                            x[X(p, a, e)] = xa - shift
                            x[X(p, b, e)] = xb + shift
                            chip_k[p * N_CHIP + a] = ka - shift
                            chip_k[p * N_CHIP + b] = kb + shift

    def worst(i, acc):
        p = i // N_CHIP
        away = p // 2 != i % N_CHIP
        return jnp.maximum(acc, jnp.where(away, chip_k[i], 0))

    top = lax.fori_loop(0, N_DEV * N_CHIP, worst, i32(0))
    pick = i32(0)
    for g in CAP_GRPS[:-1]:
        pick = pick + (top > 2 * g).astype(i32)
    pick_ref[0] = pick

    @pl.when(pick < len(CAP_GRPS) - 1)
    def _():
        room = i32(0)
        for i, g in enumerate(CAP_GRPS[:-1]):
            room = jnp.where(pick == i, 2 * g, room)
        for c in range(N_CHIP):
            def add(p, acc, c=c):
                return acc + chip_k[p * N_CHIP + c]
            loads[c] = lax.fori_loop(0, N_DEV, add, i32(0))

        @pl.loop(0, N_DEV)
        def _(p):
            own = p // 2

            @pl.loop(0, N_EXP)
            def _(e):
                @pl.when(opts[e] > 1)
                def _():
                    for a in range(N_CHIP):
                        for b in range(a + 1, N_CHIP):
                            both = (has[a * N_EXP + e] > 0) & (has[b * N_EXP + e] > 0)

                            @pl.when(both)
                            def _(a=a, b=b):
                                ka = chip_k[p * N_CHIP + a]
                                kb = chip_k[p * N_CHIP + b]
                                xa = x[X(p, a, e)]
                                xb = x[X(p, b, e)]
                                free_a = jnp.where(own == a, AID, room - ka)
                                free_b = jnp.where(own == b, AID, room - kb)
                                shift = lax.shift_right_arithmetic(loads[a] - loads[b], i32(1))
                                shift = jnp.minimum(shift, jnp.minimum(xa, free_b))
                                shift = jnp.maximum(shift, -jnp.minimum(xb, free_a))
                                x[X(p, a, e)] = xa - shift
                                x[X(p, b, e)] = xb + shift
                                chip_k[p * N_CHIP + a] = ka - shift
                                chip_k[p * N_CHIP + b] = kb + shift
                                loads[a] = loads[a] - shift
                                loads[b] = loads[b] + shift

    @pl.when(pick == len(CAP_GRPS) - 1)
    def _():
        @pl.loop(0, N_DEV * N_EXP)
        def _(i):
            p = i // N_EXP
            e = i % N_EXP
            g = grp[i]
            n = opts[e]
            done = i32(0)
            share = i32(0)
            for c in range(N_CHIP):
                done = done + has[c * N_EXP + e]
                upto = (g * done) // n
                x[X(p, c, e)] = upto - share
                share = upto

        chip_sums()

    def half(k):
        return (k + 1) // 2

    @pl.loop(0, N_EXP)
    def _(e):
        def before(c):
            def add(f, acc):
                return acc + jnp.where(f < e, x[X(me, c, f)], 0)
            return lax.fori_loop(0, N_EXP, add, i32(0))

        row = i32(0)
        prev = i32(0)

        def put(i, at, to):
            piece_at[i * N_EXP + e] = at * GROUP
            piece_add[i * N_EXP + e] = to - at * GROUP

        put(0, i32(0), before(chip) * GROUP)
        row = x[X(me, chip, e)]
        for step in range(1, N_CHIP):
            c = chip ^ step
            amt = x[X(me, c, e)]
            off = before(c)
            h0 = half(chip_k[me * N_CHIP + c])
            n0 = jnp.minimum(jnp.maximum(h0 - off, 0), amt)
            d0 = (2 * c) ^ me
            d1 = (2 * c + 1) ^ me
            put(2 * step - 1, row, cls_ref[d0] * AID * GROUP + off * GROUP)
            put(2 * step, row + n0, cls_ref[d1] * AID * GROUP + (off + n0 - h0) * GROUP)
            row = row + amt

    def expert_of(u):
        dev = me ^ (u // N_SLOT)
        return slot_ref[dev * N_SLOT + u % N_SLOT]

    def fresh_unit(u):
        e = expert_of(u)
        ok = jnp.bool_(True)
        for v in range(u):
            ok = ok & (expert_of(v) != e)
        return e, ok

    def close(call, u, first, ptr):
        t0 = first // TILE_G
        t1 = (ptr + TILE_G - 1) // TILE_G

        @pl.loop(t0, t1)
        def _(t):
            units[call][t] = i32(u)
            cnts[call][t] = jnp.minimum(ptr - t * TILE_G, TILE_G)

        return t1 * TILE_G

    ptr = i32(0)
    own_tiles = i32(0)
    for u in range(2 * N_SLOT):
        e, ok = fresh_unit(u)

        def before(f, acc, e=e):
            return acc + jnp.where(f < e, x[X(me, chip, f)], 0)

        base = lax.fori_loop(0, N_EXP, before, i32(0))
        n = jnp.where(ok, x[X(me, chip, e)], 0)

        @pl.loop(0, n)
        def _(m, ptr=ptr, base=base):
            ents[0][ptr + m] = base + m

        ptr = close(0, u, ptr, ptr + n)
        if u == N_SLOT - 1:
            own_tiles = ptr // TILE_G
    all_tiles = ptr // TILE_G

    for b, classes in enumerate(BATCHES):
        call = 1 + b
        ptr = i32(0)
        for u in range(2 * N_SLOT):
            e, ok = fresh_unit(u)
            first = ptr
            for aid, ci in enumerate(classes):
                p = me ^ CLASSES[ci]

                def before(f, acc, e=e, p=p):
                    return acc + jnp.where(f < e, x[X(p, chip, f)], 0)

                beg = lax.fori_loop(0, N_EXP, before, i32(0))
                end = beg + x[X(p, chip, e)]
                k = chip_k[p * N_CHIP + chip]
                lo = jnp.where(core == 0, 0, half(k))
                hi = jnp.where(core == 0, half(k), k)
                beg = jnp.maximum(beg, lo)
                n = jnp.where(ok, jnp.maximum(jnp.minimum(end, hi) - beg, 0), 0)

                @pl.loop(0, n)
                def _(m, ptr=ptr, beg=beg, lo=lo, aid=aid, call=call):
                    ents[call][ptr + m] = beg - lo + m + aid * AID

                ptr = ptr + n
            ptr = close(call, u, first, ptr)
        ranges[2 * b + 1][0] = i32(0)
        ranges[2 * b + 1][1] = ptr // TILE_G

    def cost(call, t):
        return TILE_COST + (cnts[call][t] * ROW_COST) // TILE_G

    done = i32(0)
    spent = i32(0)
    for b, goal in enumerate(GOALS):
        def add(t, acc, b=b):
            return acc + cost(1 + b, t)

        batch = lax.fori_loop(0, ranges[2 * b + 1][1], add, i32(0))
        limit = own_tiles if b == 0 else all_tiles

        def fill(t, carry, room=goal - (batch if b else 0)):
            upto, used = carry
            more = used < room
            return upto + more.astype(i32), used + jnp.where(more, cost(0, t), 0)

        upto, spent = lax.fori_loop(done, jnp.maximum(limit, done), fill, (done, spent))
        ranges[2 * b][0] = done
        ranges[2 * b][1] = upto
        done = upto
        spent = spent + batch
    ranges[N_RANGE - 1][0] = done
    ranges[N_RANGE - 1][1] = all_tiles


def make_plan(counts, slot_expert, me):
    smem = pl.BlockSpec(memory_space=pltpu.SMEM)
    vec = lambda n: jax.ShapeDtypeStruct((n,), jnp.int32)
    s = lambda n: pltpu.SMEM((n,), jnp.int32)
    cls = jnp.array([1 + CLASSES.index(d) if d in CLASSES else 0 for d in range(N_DEV)], jnp.int32)
    outs = [vec(N_PIECE * N_EXP)] * 2 + [vec(1)] + [vec(MAX_E)] * N_CALL + [vec(MAX_T)] * (2 * N_CALL) + [vec(2)] * N_RANGE
    res = pl.pallas_call(
        plan_kernel,
        out_shape=outs,
        in_specs=[smem] * 4,
        out_specs=[smem] * len(outs),
        scratch_shapes=[s(64), s(32), s(8), s(32), s(8), s(256)],
        name='plan',
    )(me.reshape(1), counts.reshape(-1), slot_expert.reshape(-1), cls)
    tabs = [[res[3 + k * N_CALL + i] for k in range(3)] for i in range(N_CALL)]
    return res[0], res[1], res[2], tabs, res[3 + 3 * N_CALL:]


def ffn_kernel(ent, unit, cnt, span, idx, *refs, n_src, n_pair, by_row):
    srcs, refs = refs[:n_src], refs[n_src:]
    pairs, refs = refs[:2 * n_pair], refs[2 * n_pair:]
    if by_row:
        refs = refs[1:]
    outs, refs = refs[:n_src], refs[n_src:]
    xbuf, xt, obuf, ubuf, dbuf, acc, xsem, osem, wsem = refs
    first = span[0]
    nt = span[1] - first
    nf = pairs[0].shape[3] // TILE_F
    depth = ubuf.shape[0]

    def weight_copies(s, fn):
        k = s // nf
        f = pl.multiple_of((s - k * nf) * TILE_F, TILE_F)
        b = s % depth
        u = unit[first + k]
        slot = u % N_SLOT
        for w in range(n_pair):
            def go(w=w):
                fn(pltpu.make_async_copy(pairs[2 * w].at[0, slot, :, pl.ds(f, TILE_F)], ubuf.at[b], wsem.at[b, 0]))
                fn(pltpu.make_async_copy(pairs[2 * w + 1].at[0, slot, pl.ds(f, TILE_F), :], dbuf.at[b], wsem.at[b, 1]))
            if n_pair == 1:
                go()
            else:
                pl.when(u // N_SLOT == w)(go)

    def weights_wait(s):
        b = s % depth
        pltpu.make_async_copy(pairs[0].at[0, 0, :, pl.ds(0, TILE_F)], ubuf.at[b], wsem.at[b, 0]).wait()
        pltpu.make_async_copy(pairs[1].at[0, 0, pl.ds(0, TILE_F), :], dbuf.at[b], wsem.at[b, 1]).wait()

    def x_start(k):
        b = k % 2
        t = first + k

        @pl.loop(0, cnt[t])
        def _(m):
            v = ent[t * TILE_G + m]
            if by_row:
                for r in range(GROUP):
                    pltpu.make_async_copy(srcs[0].at[idx[v * GROUP + r]], xbuf.at[b, m * GROUP + r], xsem.at[b]).start()
            else:
                for a in range(n_src):
                    @pl.when(v // AID == a)
                    def _(a=a):
                        pltpu.make_async_copy(srcs[a].at[pl.ds((v % AID) * GROUP, GROUP)], xbuf.at[b, pl.ds(m * GROUP, GROUP)], xsem.at[b]).start()

    def x_wait(k):
        b = k % 2

        @pl.loop(0, cnt[first + k])
        def _(m):
            pltpu.make_async_copy(srcs[0].at[pl.ds(0, GROUP)], xbuf.at[b, pl.ds(0, GROUP)], xsem.at[b]).wait()

    def o_start(k):
        b = k % 2
        t = first + k

        @pl.loop(0, cnt[t])
        def _(m):
            v = ent[t * TILE_G + m]
            for a in range(n_src):
                @pl.when(v // AID == a)
                def _(a=a):
                    pltpu.make_async_copy(obuf.at[b, pl.ds(m * GROUP, GROUP)], outs[a].at[pl.ds((v % AID) * GROUP, GROUP)], osem.at[b]).start()

    def o_wait(k):
        b = k % 2

        @pl.loop(0, cnt[first + k])
        def _(m):
            pltpu.make_async_copy(obuf.at[b, pl.ds(0, GROUP)], outs[0].at[pl.ds(0, GROUP)], osem.at[b]).wait()

    @pl.when(nt > 0)
    def _():
        for s in range(depth - 1):
            weight_copies(s, lambda c: c.start())
        x_start(0)

    @pl.loop(0, nt)
    def _(k):
        x_wait(k)
        xt[...] = xbuf[k % 2].reshape(xt.shape)
        acc[...] = jnp.zeros_like(acc)

        @pl.when(k + 1 < nt)
        def _():
            x_start(k + 1)

        @pl.when(k >= 1)
        def _():
            o_start(k - 1)

        rows = cnt[first + k] * GROUP

        @pl.loop(0, nf)
        def _(j):
            s = k * nf + j
            weights_wait(s)

            @pl.when(s + depth - 1 < nt * nf)
            def _():
                weight_copies(s + depth - 1, lambda c: c.start())

            b = s % depth

            def run(m):
                pre = jnp.dot(xt[:m, :], ubuf[b], preferred_element_type=jnp.float32)
                bend = jnp.tanh(pre * (GELU_A + GELU_B * (pre * pre)))
                hid = (0.5 * pre * (1.0 + bend)).astype(jnp.bfloat16)
                acc[:m, :] += jnp.dot(hid, dbuf[b], preferred_element_type=jnp.float32)

            for m in SIZES:
                lo = max([v for v in SIZES if v < m], default=0)
                pl.when((rows > lo) & (rows <= m))(functools.partial(run, m))

        @pl.when(k >= 2)
        def _():
            o_wait(k - 2)

        obuf[k % 2] = acc[...].astype(jnp.bfloat16).reshape(obuf.shape[1:])

    @pl.when(nt >= 1)
    def _():
        @pl.when(nt >= 2)
        def _():
            o_wait(nt - 2)

        o_start(nt - 1)
        o_wait(nt - 1)


def ffn(tab, span, idx, srcs, pairs, back, name):
    by_row = back is not None
    ent, unit, cnt = tab
    flat = [w for pair in pairs for w in pair]
    d = flat[0].shape[2]
    f = flat[0].shape[3]
    any_spec = pl.BlockSpec(memory_space=pl.ANY)
    n_src = len(srcs)
    extra = [back] if by_row else []
    shapes = [jax.ShapeDtypeStruct(a.shape, a.dtype) for a in ([back] if by_row else srcs)]
    row = (d // LANE, LANE)
    rows_est = 2048
    smem = pl.BlockSpec(memory_space=pltpu.SMEM)
    return pl.pallas_call(
        functools.partial(ffn_kernel, n_src=n_src, n_pair=len(pairs), by_row=by_row),
        in_specs=[smem] * 5 + [any_spec] * (n_src + len(flat) + len(extra)),
        out_specs=[any_spec] * n_src,
        scratch_shapes=[
            pltpu.VMEM((2, TILE_M) + row, jnp.bfloat16),
            pltpu.VMEM((TILE_M, d), jnp.bfloat16),
            pltpu.VMEM((2, TILE_M) + row, jnp.bfloat16),
            pltpu.VMEM((DEPTH, d, TILE_F), jnp.bfloat16),
            pltpu.VMEM((DEPTH, TILE_F, d), jnp.bfloat16),
            pltpu.VMEM((TILE_M, d), jnp.float32),
            pltpu.SemaphoreType.DMA((2,)),
            pltpu.SemaphoreType.DMA((2,)),
            pltpu.SemaphoreType.DMA((DEPTH, 2)),
        ],
        out_shape=shapes,
        input_output_aliases={5 + n_src + len(flat): 0} if by_row else {},
        compiler_params=pltpu.CompilerParams(vmem_limit_bytes=VMEM_BYTES),
        cost_estimate=pl.CostEstimate(flops=4 * rows_est * d * f, bytes_accessed=100_000_000, transcendentals=rows_est * f),
        name=name,
    )(ent, unit, cnt, span, idx, *srcs, *flat, *extra)


def pick_kernel(idx, src, *refs, per):
    outs, (buf, sem) = refs[:-2], refs[-2:]
    t = pl.program_id(0)
    n = pl.num_programs(0)
    rows = outs[0].shape[0]

    def start(k):
        @pl.loop(0, rows // 8)
        def _(m):
            for r in range(8):
                q = m * 8 + r
                pltpu.make_async_copy(src.at[idx[k * rows + q]], buf.at[k % 2, q], sem.at[k % 2]).start()

    pl.when(t == 0)(lambda: start(t))
    pl.when(t + 1 < n)(lambda: start(t + 1))
    pltpu.make_async_copy(src.at[pl.ds(0, rows)], buf.at[t % 2], sem.at[t % 2]).wait()
    for c, o in enumerate(outs):
        @pl.when(t // per == c)
        def _(o=o):
            o[...] = buf[t % 2]


def pick_rows(src, idx, n_out, name):
    row = src.shape[1:]
    n = idx.shape[0] // n_out
    per = 2
    tile = n // per

    def spec(c):
        return pl.BlockSpec((tile,) + row, lambda t, s: (jnp.clip(t - c * per, 0, per - 1), 0, 0))

    return pl.pallas_call(
        functools.partial(pick_kernel, per=per),
        grid_spec=pltpu.PrefetchScalarGridSpec(
            num_scalar_prefetch=1,
            grid=(per * n_out,),
            in_specs=[pl.BlockSpec(memory_space=pl.ANY)],
            out_specs=[spec(c) for c in range(n_out)],
            scratch_shapes=[pltpu.VMEM((2, tile) + row, src.dtype), pltpu.SemaphoreType.DMA((2,))],
        ),
        out_shape=[jax.ShapeDtypeStruct((n,) + row, src.dtype)] * n_out,
        compiler_params=pltpu.CompilerParams(vmem_limit_bytes=VMEM_BYTES),
        name=name,
    )(idx, src)


def mix_kernel(p0, p1, src, w, o_ref, buf, sem):
    t = pl.program_id(0)
    n = pl.num_programs(0)
    rows = o_ref.shape[0]

    def start(k):
        @pl.loop(0, rows // 4)
        def _(m):
            for r in range(4):
                q = m * 4 + r
                pltpu.make_async_copy(src.at[p0[k * rows + q]], buf.at[k % 2, 0, q], sem.at[k % 2, 0]).start()
                pltpu.make_async_copy(src.at[p1[k * rows + q]], buf.at[k % 2, 1, q], sem.at[k % 2, 1]).start()

    pl.when(t == 0)(lambda: start(t))
    pl.when(t + 1 < n)(lambda: start(t + 1))
    for h in range(2):
        pltpu.make_async_copy(src.at[pl.ds(0, rows)], buf.at[t % 2, h], sem.at[t % 2, h]).wait()
    a, b = (buf[t % 2, h].reshape(o_ref.shape).astype(jnp.float32) for h in range(2))
    o_ref[...] = (a * w[:, :1] + b * w[:, 1:]).astype(o_ref.dtype)


def mix(back, pos, topk_w):
    row = back.shape[1:]
    n = pos[0].shape[0]
    d = row[0] * row[1]
    tile = 256
    w_spec = pl.BlockSpec((tile, topk_w.shape[1]), lambda t, a, b: (t, 0))
    return pl.pallas_call(
        mix_kernel,
        grid_spec=pltpu.PrefetchScalarGridSpec(
            num_scalar_prefetch=2,
            grid=(n // tile,),
            in_specs=[pl.BlockSpec(memory_space=pl.ANY), w_spec],
            out_specs=pl.BlockSpec((tile, d), lambda t, a, b: (t, 0)),
            scratch_shapes=[pltpu.VMEM((2, 2, tile) + row, back.dtype), pltpu.SemaphoreType.DMA((2, 2))],
        ),
        out_shape=jax.ShapeDtypeStruct((n, d), back.dtype),
        compiler_params=pltpu.CompilerParams(vmem_limit_bytes=VMEM_BYTES),
        name='mix',
    )(pos[0], pos[1], back, topk_w)


def fresh(shape):
    return pl.pallas_call(lambda o: None, out_shape=jax.ShapeDtypeStruct(shape, jnp.bfloat16), out_specs=pl.BlockSpec(memory_space=pl.ANY), name='fresh')()


def count_pairs(topk_idx):
    experts = jnp.arange(N_EXP, dtype=jnp.int32)
    hits = [topk_idx[:, j][None, :] == experts[:, None] for j in range(topk_idx.shape[1])]
    one = sum(h.astype(jnp.int32) for h in hits)
    incl = jnp.cumsum(one, axis=1)
    return hits, incl - one, incl[:, -1]


def invert(pos, n_rows):
    n_tok = pos[0].shape[0]
    lo_n = 64
    hi_ids = jnp.arange(n_rows // lo_n, dtype=jnp.int32)
    lo_ids = jnp.arange(2 * lo_n, dtype=jnp.int32)
    tok = jnp.arange(n_tok, dtype=jnp.int32)
    val = jnp.where(lo_ids[None, :] < lo_n, (tok // lo_n)[:, None] + 1, (tok % lo_n)[:, None])
    packed = 0.0
    for p in pos:
        left = ((p // lo_n)[None, :] == hi_ids[:, None]).astype(jnp.bfloat16)
        right = jnp.where((p % lo_n)[:, None] == (lo_ids % lo_n)[None, :], val, 0).astype(jnp.bfloat16)
        packed = packed + jnp.dot(left, right, preferred_element_type=jnp.float32)
    packed = packed.astype(jnp.int32)
    spare = (hi_ids[:, None] * lo_n + jnp.arange(lo_n, dtype=jnp.int32)[None, :]) % n_tok
    return jnp.where(packed[:, :lo_n] > 0, (packed[:, :lo_n] - 1) * lo_n + packed[:, lo_n:], spare).reshape(-1)


def swap(a, d):
    return lax.ppermute(a, 'ep', [(p, p ^ d) for p in range(N_DEV)])


def layer_branch(cap_grps, tok3, pos_virtual, topk_w, w_up, w_down, tabs, spans):
    cap = cap_grps * GROUP
    local = LOCAL_GRPS * GROUP
    row = tok3.shape[1:]
    n_cls = len(CLASSES)
    span = AID * GROUP
    pos = []
    for v in pos_virtual:
        ci = v // span
        pos.append(jnp.where(ci == 0, v, local + (ci - 1) * cap + v % span))
    total = local + n_cls * cap
    idx = invert(pos, (total + 63) // 64 * 64)
    own = (w_up, w_down)
    picked = []
    part = idx[local:local + len(BATCHES[0]) * cap]
    for b, classes in enumerate(BATCHES):
        got = list(pick_rows(tok3, part, len(classes), f'pick{b}'))
        if b + 1 < len(BATCHES):
            lo = local + BATCHES[b + 1][0] * cap
            part, got[-1] = lax.optimization_barrier((idx[lo:lo + len(BATCHES[b + 1]) * cap], got[-1]))
        picked.append(got)
    up, down, _ = lax.optimization_barrier((w_up, w_down, picked[-1][-1]))
    sib = (swap(up, 1), swap(down, 1))
    sent = [swap(g, CLASSES[ci]) for g, ci in zip(picked[0], BATCHES[0])]
    loc_idx = idx[:local]
    back = fresh((total,) + row)
    home = [None] * n_cls
    for b, classes in enumerate(BATCHES):
        if b:
            back, _ = lax.optimization_barrier((back, outs[0]))
        (back,) = ffn(tabs[0], spans[2 * b], loc_idx, [tok3], [own, sib][:1 + b], back, f'ffn_l{b}')
        if b + 1 < len(BATCHES):
            back, ready, later = lax.optimization_barrier((back, sent[-len(classes):], picked[b + 1]))
            sent[-len(classes):] = ready
            sent += [swap(g, CLASSES[ci]) for g, ci in zip(later, BATCHES[b + 1])]
        ent, back = lax.optimization_barrier((tabs[1 + b][0], back))
        outs = ffn([ent] + tabs[1 + b][1:], spans[2 * b + 1], loc_idx[:8], [sent[ci] for ci in classes], [own, sib], None, f'ffn_b{b}')
        for ci, o in zip(classes, outs):
            home[ci] = swap(o, CLASSES[ci])
    back, _ = lax.optimization_barrier((back, outs[0]))
    (back,) = ffn(tabs[0], spans[-1], loc_idx, [tok3], [own, sib], back, 'ffn_end')
    for ci in range(n_cls):
        back = lax.dynamic_update_slice(back, home[ci], (local + ci * cap, 0, 0))
    return mix(back, pos, topk_w)


def solution(mesh):
    def group_layer(tokens, topk_idx, topk_w, w_up, w_down, slot_expert):
        n_tok, d = tokens.shape
        me = lax.axis_index('ep').astype(jnp.int32)
        hits, rank, counts = count_pairs(topk_idx)
        all_counts = lax.all_to_all(jnp.broadcast_to(counts, (N_DEV, N_EXP)), 'ep', 0, 0, tiled=True)
        tok3, all_counts = lax.optimization_barrier((tokens.reshape(n_tok, d // LANE, LANE), all_counts))
        at, add, pick, tabs, spans = make_plan(all_counts, slot_expert, me)
        at = at.reshape(N_PIECE, N_EXP, 1)
        add = add.reshape(N_PIECE, N_EXP, 1)
        place = rank + add[0]
        for i in range(1, N_PIECE):
            place = jnp.where(rank >= at[i], rank + add[i], place)
        pos = [jnp.sum(jnp.where(h, place, 0), axis=0) for h in hits]
        branches = [functools.partial(layer_branch, g) for g in CAP_GRPS]
        return lax.switch(pick[0], branches, tok3, pos, topk_w, w_up, w_down, tabs, spans)

    row_spec = P(('dp', 'ep'), None)
    weight_spec = P('ep', None, None, None)
    return jax.shard_map(group_layer, mesh=mesh, in_specs=(row_spec, row_spec, row_spec, weight_spec, weight_spec, P(None, None)), out_specs=row_spec, check_vma=False)
```
